32 devices in a mesh: frame: 16 (over z, x, core), tok: 2 (over y).
Axes of the slice: x: 2, y: 2, z: 4, core: 2. Of those that a mesh axis runs over, the one named last changes fastest.
Arguments:
- queries: bfloat16 [16, 256, 1024], P('frame', 'tok'), may hold values from -40 to 40
- key_rows: bfloat16 [16, 256, 1024], P('frame', 'tok'), may hold values from -40 to 40
- value_rows: bfloat16 [16, 256, 1024], P('frame', 'tok'), may hold values from -6 to 6
- grad_out: bfloat16 [16, 256, 1024], P('frame', 'tok'), may hold values from -6 to 6
- video_of_frame: int32 [16], replicated, may hold values from 0 to 5, never falling along the last dimension, each value on 1 to 4 neighbouring positions
- age_pool: int32 [3], replicated, may hold values from 2 to 8, as said below
Outputs:
- attention_out: bfloat16 [16, 256, 1024], P('frame', 'tok')
- grad_queries: bfloat16 [16, 256, 1024], P('frame', 'tok')
- grad_keys: bfloat16 [16, 256, 1024], P('frame', 'tok')
- grad_values: bfloat16 [16, 256, 1024], P('frame', 'tok')
The draws below stay inside these ranges and needn't reach their ends.
Inputs may be any that keep to these rules, and one draw needn't show every extreme that they name: `video_of_frame`: video ids never fall along the frames; every video holds 1 to 4 frames. `age_pool`: each entry is 2, 4 or 8, and each of the three appears; entry a - 1 is the factor of a frame a frames older.
All inputs are finite; a program needn't handle non-finite values.
Results may differ from the reference program's by a relative error of at most 0.025.
Values may be sent and summed in bfloat16 or wider, within the bound.
No kernel may reach another device: no remote copies, remote signals or barrier semaphores. Data moves between devices by JAX's collectives and lax.ppermute only.
A program may use at most 64 MiB of HBM per device.

```python
import math
import jax
import jax.numpy as jnp
import numpy as np
from jax import lax

HEADS = 16
HEAD = 64
HIST = 3
FRAME_TOKENS = 256
FRAMES = 16
VIDEOS = 6


def paired_draw(key):
    columns = HEADS * HEAD
    shape = (FRAMES, FRAME_TOKENS, columns)
    query_draw = jnp.clip(jax.random.normal(jax.random.fold_in(key, 101), shape, jnp.float32), -6.0, 6.0)
    key_draw = jnp.clip(jax.random.normal(jax.random.fold_in(key, 102), shape, jnp.float32), -6.0, 6.0)
    return (query_draw, key_draw)


def draw_queries(key, part):
    return paired_draw(key)[0].astype(jnp.bfloat16)


def draw_key_rows(key, part):
    return paired_draw(key)[1].astype(jnp.bfloat16)


def draw_age_pool(key, part):
    cycle = (jnp.arange(HIST, dtype=jnp.int32) % 3 + 1).astype(jnp.int32)
    powers = jax.random.permutation(jax.random.fold_in(key, 201), cycle)
    return jnp.left_shift(jnp.ones((HIST,), jnp.int32), powers.astype(jnp.int32)).astype(jnp.int32)


def block_scale(stream_key, extent, cuts, low, high):
    level = 1.0
    for dim, parts in cuts:
        heights = jax.random.uniform(jax.random.fold_in(jax.random.fold_in(stream_key, 6), dim), (parts,), jnp.float32, low / len(cuts), high / len(cuts))
        level = level * jnp.repeat(jnp.exp(heights), extent[dim] // parts).reshape((-1,) + (1,) * (len(extent) - 1 - dim))
    return level


def split_up(amount, total, reach, slope):
    loads = [(1 << 20) // math.isqrt(grade ** slope) + 1 for grade in range(2, amount + 1)]
    rest, counts = total - reach - (amount - 1), [1] * (amount - 1)
    while rest > 0:
        free = [i for i in range(amount - 1) if counts[i] < reach]
        pool, left = sum([loads[i] for i in free]), rest
        for i in free:
            more = min(reach - counts[i], max(1, left * loads[i] // pool), rest)
            counts[i] = counts[i] + more
            rest = rest - more
    return np.array([reach] + counts)


def ragged_sizes(stream_key, amount, total, reach, lean):
    if amount == 2:
        one = jax.random.randint(stream_key, (), max(1, total - reach), min(reach, total - 1) + 1)
        return jnp.stack([one, total - one])
    tallies = jnp.asarray(split_up(amount, total, reach, lean), jnp.int32)
    pairs = (amount - 1) // 2
    giver, receiver = tallies[1:1 + 2 * pairs:2], tallies[2:2 + 2 * pairs:2]
    room = jnp.minimum(giver - 1, reach - receiver)
    shifted = jax.random.randint(jax.random.fold_in(stream_key, 1), (pairs,), 0, 1 << 20) % (room + 1)
    tallies = tallies.at[1:1 + 2 * pairs:2].set(giver - shifted).at[2:2 + 2 * pairs:2].set(receiver + shifted)
    return tallies[jax.random.permutation(jax.random.fold_in(stream_key, 2), amount)]


def noise(rng, dims, deviation, most, shards=(), kind=jnp.bfloat16):
    values = jax.random.normal(rng, dims, jnp.float32) * deviation
    if len(shards) > 0:
        values = block_scale(rng, dims, shards, -0.22, 0.18) * values
    return jnp.clip(values, min=-most, max=most).astype(kind)


def setup_inputs(seed: int = 0) -> dict:
    splits = jax.random.split(jax.random.key(seed), 7)
    return {
        "queries": draw_queries(jax.random.fold_in(splits[6], 71), 0),
        "key_rows": draw_key_rows(jax.random.fold_in(splits[6], 71), 0),
        "value_rows": noise(splits[2], (FRAMES, FRAME_TOKENS, HEADS * HEAD), 1.0, 6.0, ((0, 16), (1, 2))),
        "grad_out": noise(splits[3], (FRAMES, FRAME_TOKENS, HEADS * HEAD), 1.0, 6.0, ((0, 16), (1, 2))),
        "video_of_frame": jnp.searchsorted(jnp.cumsum(ragged_sizes(splits[4], VIDEOS, FRAMES, HIST + 1, 0)), jnp.arange(FRAMES), side="right").astype(jnp.int32),
        "age_pool": draw_age_pool(jax.random.fold_in(splits[6], 71), 0),
    }


def pooled_pick(source_rows, factor):
    total_rows, columns = source_rows.shape
    half_rows = total_rows // 2
    picked = jnp.zeros((half_rows, columns), jnp.float32)
    for stride in (2, 4, 8):
        average = source_rows.astype(jnp.float32).reshape(total_rows // stride, stride, columns).mean(axis=1)
        padded = jnp.pad(average, ((0, half_rows - total_rows // stride), (0, 0)))
        picked = jnp.where(factor == stride, padded, picked)
    return picked.astype(jnp.bfloat16)


def spread_back(pooled_grads, factor, total_rows):
    columns = pooled_grads.shape[1]
    widened = jnp.zeros((total_rows, columns), jnp.float32)
    for stride in (2, 4, 8):
        portion = pooled_grads[: total_rows // stride]
        spread = jnp.broadcast_to(portion[:, None, :], (total_rows // stride, stride, columns)).reshape(total_rows, columns) / stride
        widened = jnp.where(factor == stride, spread, widened)
    return widened


def attend_block(query_block, key_set, value_set, key_mask, grad_block, scaling):
    query_wide = query_block.astype(jnp.float32)
    key_wide = key_set.astype(jnp.float32)
    value_wide = value_set.astype(jnp.float32)
    grad_wide = grad_block.astype(jnp.float32)
    scores = jnp.einsum("qhd,khd->hqk", query_wide, key_wide) * scaling
    scores = jnp.where(key_mask[None, None, :], scores, -jnp.inf)
    highest = jnp.max(scores, axis=2, keepdims=True)
    exponent = jnp.exp(scores - highest)
    weights = exponent / jnp.sum(exponent, axis=2, keepdims=True)
    rounded = weights.astype(jnp.bfloat16)
    output = jnp.einsum("hqk,khd->qhd", rounded.astype(jnp.float32), value_wide).astype(jnp.bfloat16)
    inner_sum = jnp.sum(grad_wide * output.astype(jnp.float32), axis=2).T[:, :, None]
    grad_weights = jnp.einsum("qhd,khd->hqk", grad_wide, value_wide)
    grad_scores = (weights * (grad_weights - inner_sum)).astype(jnp.bfloat16)
    scores_wide = grad_scores.astype(jnp.float32)
    grad_query = jnp.einsum("hqk,khd->qhd", scores_wide, key_wide) * scaling
    grad_key_set = jnp.einsum("hqk,qhd->khd", scores_wide, query_wide) * scaling
    grad_value_set = jnp.einsum("hqk,qhd->khd", rounded.astype(jnp.float32), grad_wide)
    return output, grad_query, grad_key_set, grad_value_set


def reference(queries, key_rows, value_rows, grad_out, video_of_frame, age_pool):
    scaling = HEAD ** -0.5
    half_rows = FRAME_TOKENS // 2
    columns = HEADS * HEAD

    def frame_step(totals, frame_index):
        key_total, value_total = totals
        key_parts = [key_rows[frame_index]]
        value_parts = [value_rows[frame_index]]
        mask_parts = [jnp.ones((FRAME_TOKENS,), jnp.bool_)]
        sources = []
        for offset in range(1, HIST + 1):
            factor = age_pool[offset - 1]
            source = jnp.maximum(frame_index - offset, 0).astype(jnp.int32)
            usable = (frame_index >= offset) & (video_of_frame[source] == video_of_frame[frame_index])
            key_parts.append(pooled_pick(key_rows[source], factor))
            value_parts.append(pooled_pick(value_rows[source], factor))
            mask_parts.append(usable & (jnp.arange(half_rows) < FRAME_TOKENS // factor))
            sources.append(source)
        key_set = jnp.concatenate(key_parts, axis=0).reshape(-1, HEADS, HEAD)
        value_set = jnp.concatenate(value_parts, axis=0).reshape(-1, HEADS, HEAD)
        key_mask = jnp.concatenate(mask_parts)
        output, grad_query, grad_key_set, grad_value_set = attend_block(
            queries[frame_index].reshape(FRAME_TOKENS, HEADS, HEAD), key_set, value_set, key_mask,
            grad_out[frame_index].reshape(FRAME_TOKENS, HEADS, HEAD), scaling)
        grad_key_set = grad_key_set.reshape(-1, columns)
        grad_value_set = grad_value_set.reshape(-1, columns)
        key_total = key_total.at[frame_index].add(grad_key_set[:FRAME_TOKENS])
        value_total = value_total.at[frame_index].add(grad_value_set[:FRAME_TOKENS])
        for offset in range(1, HIST + 1):
            factor = age_pool[offset - 1]
            start_row = FRAME_TOKENS + (offset - 1) * half_rows
            key_total = key_total.at[sources[offset - 1]].add(spread_back(grad_key_set[start_row:start_row + half_rows], factor, FRAME_TOKENS))
            value_total = value_total.at[sources[offset - 1]].add(spread_back(grad_value_set[start_row:start_row + half_rows], factor, FRAME_TOKENS))
        return (key_total, value_total), (output.reshape(FRAME_TOKENS, columns), grad_query.reshape(FRAME_TOKENS, columns).astype(jnp.bfloat16))

    zero_grads = jnp.zeros((FRAMES, FRAME_TOKENS, columns), jnp.float32)
    (key_total, value_total), (attention_out, grad_queries) = lax.scan(frame_step, (zero_grads, zero_grads), jnp.arange(FRAMES, dtype=jnp.int32))
    return attention_out, grad_queries, key_total.astype(jnp.bfloat16), value_total.astype(jnp.bfloat16)
```

```python
from functools import partial
import math

import jax
import jax.numpy as jnp
from jax import lax
from jax.experimental import pallas as pl
from jax.experimental.pallas import tpu as pltpu
from jax.sharding import PartitionSpec as P

HEAD = 64
POOLS = (2, 4, 8)
ORDERS = ((1, 2, 3), (1, 3, 2), (2, 1, 3), (2, 3, 1), (3, 1, 2), (3, 2, 1))
LANES = 128
FAR = -1e30
BF = jnp.bfloat16
F32 = jnp.float32
VM = pl.BlockSpec(memory_space=pltpu.VMEM)
SM = pl.BlockSpec(memory_space=pltpu.SMEM)


def shape_of(*dims, dtype=BF):
    return jax.ShapeDtypeStruct(dims, dtype)


def call(body, outs, specs, flops=1 << 20):
    return pl.pallas_call(
        body,
        out_shape=outs,
        in_specs=specs,
        out_specs=jax.tree.map(lambda _: VM, outs),
        cost_estimate=pl.CostEstimate(flops=flops, bytes_accessed=1 << 20, transcendentals=0),
    )


def dot(a, b, dims=((1,), (0,))):
    return lax.dot_general(a, b, (dims, ((), ())), preferred_element_type=F32)


def column(start, width):
    return pl.ds(pl.multiple_of(start, LANES), width)


def pack_body(width, first, second, packed):
    away = (1 - lax.axis_index("tok")) * width
    packed[0] = first[:, column(away, width)]
    packed[1] = second[:, column(away, width)]


def pool_matrix(rows, across=False):
    parts = []
    for factor in POOLS:
        count = rows // factor
        dims = (rows, count) if across else (count, rows)
        token = lax.broadcasted_iota(jnp.int32, dims, 0 if across else 1)
        pooled = lax.broadcasted_iota(jnp.int32, dims, 1 if across else 0)
        low = pooled * factor
        inside = (token >= low) & (token < low + factor)
        parts.append(jnp.where(inside, 1.0 / factor, 0.0).astype(F32))
    return jnp.concatenate(parts, axis=1 if across else 0).astype(BF)


def own_start(width, whole_rows):
    return lax.axis_index("tok") * width if whole_rows else 0


def pool_body(rows, width, others, whole_rows, key_own, value_own, moved, *outs):
    start = own_start(width, whole_rows)
    matrix = pool_matrix(rows)
    for which, own in enumerate((key_own, value_own)):
        for block in range(others + 1):
            if block == 0:
                source = own[:, column(start, width)]
            else:
                source = moved[which, (block - 1) * rows : block * rows, :]
            pooled = dot(matrix, source).astype(BF)
            low = 0
            for factor, out in zip(POOLS, outs):
                count = rows // factor
                out[which, block * count : (block + 1) * count, :] = pooled[low : low + count]
                low += count


def attend_body(
    rows, width, others, whole_rows,
    video, age, query_own, key_own, value_own, grad_own, moved_kv, moved_qg, *rest
):
    pooled, outs = rest[:3], rest[3:]
    out_own, dquery_own, out_moved, dkv_own = outs[:4]
    dpooled = outs[4:]
    start = own_start(width, whole_rows)
    here = lax.axis_index("frame")
    frame_rows = rows * (others + 1)
    biases = []
    for factor in POOLS:
        distance = jnp.int32(0)
        for a in range(3):
            distance = jnp.where(age[a] == factor, a + 1, distance)
        source = jnp.maximum(here - distance, 0)
        usable = (here >= distance) & (video[source] == video[here])
        biases.append(jnp.where(usable, 0.0, FAR).astype(F32))
    counts = [frame_rows // factor for factor in POOLS]
    used = frame_rows + sum(counts)
    padding = -used % LANES
    scale = HEAD**-0.5
    turn = scale * math.log2(math.e)
    block_chunks = 2 if (others + 1) % 2 == 0 else 1
    block_rows = block_chunks * rows

    def pair_step(pair, carry):
        offset = pair * LANES
        mine = column(start + offset, LANES)
        cols = column(offset, LANES)
        first_head = lax.broadcasted_iota(jnp.int32, (1, LANES), 1) < HEAD

        def key_rows_of(which, own):
            parts = [own[:, mine], moved_kv[which, :, cols]]
            parts += [p[which, :, cols] for p in pooled]
            if padding:
                parts.append(jnp.zeros((padding, LANES), BF))
            return jnp.concatenate(parts, axis=0)

        keys = key_rows_of(0, key_own)
        values = key_rows_of(1, value_own)
        keys_t = keys.T
        values_t = values.T
        dkeys = dvalues = None
        for block in range((others + 1) // block_chunks):
            chunks = range(block * block_chunks, (block + 1) * block_chunks)

            def query_rows_of(which, own):
                return jnp.concatenate(
                    [
                        own[:, mine] if c == 0 else moved_qg[which, (c - 1) * rows : c * rows, cols]
                        for c in chunks
                    ],
                    axis=0,
                )

            query = query_rows_of(0, query_own)
            grad = query_rows_of(1, grad_own)
            grad_t = grad.T
            results = []
            for head in range(2):
                keep = first_head if head == 0 else ~first_head
                query_h = jnp.where(keep, query, jnp.zeros_like(query))
                grad_h = jnp.where(keep, grad, jnp.zeros_like(grad))
                band = slice(head * HEAD, (head + 1) * HEAD)
                raw = dot(keys, query_h, ((1,), (1,)))
                parts = [raw[:frame_rows]]
                low = frame_rows
                for count, bias in zip(counts, biases):
                    parts.append(raw[low : low + count] + bias)
                    low += count
                if padding:
                    parts.append(jnp.full((padding, block_rows), FAR, F32))
                scores = jnp.concatenate(parts, axis=0)
                highest = jnp.max(scores, axis=0, keepdims=True)
                exponent = jnp.exp2((scores - highest) * turn)
                total = jnp.sum(exponent, axis=0, keepdims=True)
                weights = exponent * (1.0 / total)
                rounded = weights.astype(BF)
                out_t = dot(values_t[band], rounded).astype(BF)
                inner = jnp.sum(
                    grad_t[band].astype(F32) * out_t.astype(F32), axis=0, keepdims=True
                )
                dweights = dot(values, grad_h, ((1,), (1,)))
                dscores = (weights * (dweights - inner)).astype(BF)
                dquery_t = (dot(keys_t[band], dscores) * scale).astype(BF)
                results.append((query_h, grad_h, rounded, dscores, out_t, dquery_t))
            query_2, grad_2 = (
                jnp.concatenate([r[i] for r in results], axis=0) for i in (0, 1)
            )
            rounded_2, dscores_2 = (
                jnp.concatenate([r[i] for r in results], axis=1) for i in (2, 3)
            )
            out_2, dquery_2 = (
                jnp.concatenate([r[i] for r in results], axis=0).T for i in (4, 5)
            )
            dk = dot(dscores_2, query_2)
            dv = dot(rounded_2, grad_2)
            dkeys = dk if dkeys is None else dkeys + dk
            dvalues = dv if dvalues is None else dvalues + dv
            for place, c in enumerate(chunks):
                piece = slice(place * rows, (place + 1) * rows)
                if c == 0:
                    out_own[:, cols] = out_2[piece]
                    dquery_own[:, cols] = dquery_2[piece]
                else:
                    target = slice((c - 1) * rows, c * rows)
                    out_moved[0, target, cols] = out_2[piece]
                    out_moved[1, target, cols] = dquery_2[piece]
        for which, total in enumerate((dkeys * scale, dvalues)):
            dkv_own[which, :, cols] = total[:frame_rows]
            low = frame_rows
            for count, target in zip(counts, dpooled):
                target[which, :, cols] = total[low : low + count].astype(BF)
                low += count
        return carry

    lax.fori_loop(0, width // LANES, pair_step, 0)


def combine_body(rows, width, others, dkv_own, *rest):
    back, (dkey_own, dvalue_own, moved) = rest[:3], rest[3:]
    matrix = pool_matrix(rows, across=True)
    for which, own in enumerate((dkey_own, dvalue_own)):
        for block in range(others + 1):
            pieces = []
            for factor, ref in zip(POOLS, back):
                count = rows // factor
                pieces.append(ref[which, block * count : (block + 1) * count, :])
            spread = dot(matrix, jnp.concatenate(pieces, axis=0))
            total = (dkv_own[which, block * rows : (block + 1) * rows, :] + spread).astype(BF)
            if block == 0:
                own[...] = total
            else:
                moved[which, (block - 1) * rows : block * rows, :] = total


def unpack_body(width, *refs):
    ins, outs = refs[:6], refs[6:]
    mine = lax.axis_index("tok") * width
    away = (1 - lax.axis_index("tok")) * width
    for i, out in enumerate(outs):
        out[:, column(mine, width)] = ins[i][...]
        out[:, column(away, width)] = ins[4 + i // 2][i % 2]


def on_device(queries, key_rows, value_rows, grad_out, video_of_frame, age_pool):
    rows, columns = queries.shape[1:]
    ranks = lax.axis_size("tok")
    frames = lax.axis_size("frame")
    others = ranks - 1
    width = columns // ranks
    frame_rows = rows * ranks
    pair = ranks == 2
    swap = [(0, 1), (1, 0)]
    query, key, value, grad = (
        x.reshape(rows, columns) for x in (queries, key_rows, value_rows, grad_out)
    )
    if pair:
        pack = call(partial(pack_body, width), shape_of(2, rows, width), [VM, VM])
        moved_kv = lax.ppermute(pack(key, value), "tok", swap)
        moved_qg = lax.ppermute(pack(query, grad), "tok", swap)
    else:
        query, key, value, grad = (
            lax.all_to_all(x, "tok", split_axis=1, concat_axis=0, tiled=True)
            for x in (query, key, value, grad)
        )
        moved_kv = jnp.stack([key[rows:], value[rows:]])
        moved_qg = jnp.stack([query[rows:], grad[rows:]])
        query, key, value, grad = (x[:rows] for x in (query, key, value, grad))
    pooled_shapes = [shape_of(2, frame_rows // factor, width) for factor in POOLS]
    pooled = call(
        partial(pool_body, rows, width, others, pair), pooled_shapes, [VM] * 3
    )(key, value, moved_kv)

    where_two = jnp.where(age_pool[0] == 2, 0, jnp.where(age_pool[1] == 2, 1, 2))
    four_first = (age_pool[0] == 4) | ((age_pool[0] == 2) & (age_pool[1] == 4))
    order = (2 * where_two + jnp.where(four_first, 0, 1)).astype(jnp.int32)

    def shift(distances, sign, *blocks):
        return tuple(
            lax.ppermute(b, "frame", [(i, (i + sign * d) % frames) for i in range(frames)])
            for b, d in zip(blocks, distances)
        )

    pooled = lax.switch(order, [partial(shift, o, 1) for o in ORDERS], *pooled)
    heads = width // HEAD
    keys = frame_rows + sum(frame_rows // factor for factor in POOLS)
    results = call(
        partial(attend_body, rows, width, others, pair),
        [
            shape_of(rows, width),
            shape_of(rows, width),
            shape_of(2, others * rows, width),
            shape_of(2, frame_rows, width, dtype=F32),
            *pooled_shapes,
        ],
        [SM, SM] + [VM] * 9,
        flops=10 * frame_rows * keys * HEAD * heads,
    )(video_of_frame, age_pool, query, key, value, grad, moved_kv, moved_qg, *pooled)
    out_own, dquery_own, out_moved, dkv_own = results[:4]
    if pair:
        out_back = lax.ppermute(out_moved, "tok", swap)
    back = lax.switch(order, [partial(shift, o, -1) for o in ORDERS], *results[4:])
    dkey_own, dvalue_own, dkv_moved = call(
        partial(combine_body, rows, width, others),
        [shape_of(rows, width), shape_of(rows, width), shape_of(2, others * rows, width)],
        [VM] * 4,
    )(dkv_own, *back)
    if pair:
        dkv_back = lax.ppermute(dkv_moved, "tok", swap)
        outs = call(
            partial(unpack_body, width), [shape_of(rows, columns)] * 4, [VM] * 6
        )(out_own, dquery_own, dkey_own, dvalue_own, out_back, dkv_back)
    else:
        outs = [
            lax.all_to_all(
                jnp.concatenate([own, moved], axis=0), "tok", split_axis=0, concat_axis=1, tiled=True
            )
            for own, moved in (
                (out_own, out_moved[0]),
                (dquery_own, out_moved[1]),
                (dkey_own, dkv_moved[0]),
                (dvalue_own, dkv_moved[1]),
            )
        ]
    return tuple(x.reshape(1, rows, columns) for x in outs)


def solution(mesh):
    rows = P("frame", "tok", None)
    return jax.shard_map(
        on_device,
        mesh=mesh,
        in_specs=(rows,) * 4 + (P(), P()),
        out_specs=(rows,) * 4,
        check_vma=False,
    )
```

```python
from functools import partial
import math

import jax
import jax.numpy as jnp
from jax import lax
from jax.experimental import pallas as pl
from jax.experimental.pallas import tpu as pltpu
from jax.sharding import PartitionSpec as P


HEAD = 64
POOLS = (2, 4, 8)
ORDERS = ((1, 2, 3), (1, 3, 2), (2, 1, 3), (2, 3, 1), (3, 1, 2), (3, 2, 1))
LANES = 128
FAR = -1e30
BF = jnp.bfloat16
F32 = jnp.float32
VM = pl.BlockSpec(memory_space=pltpu.VMEM)
SM = pl.BlockSpec(memory_space=pltpu.SMEM)
ANY = pl.BlockSpec(memory_space=pl.ANY)


def shape_of(*dims, dtype=BF):
    return jax.ShapeDtypeStruct(dims, dtype)


def call(body, outs, specs, flops=1 << 20, grant=16 << 20):
    return pl.pallas_call(
        body,
        out_shape=outs,
        compiler_params=pltpu.CompilerParams(vmem_limit_bytes=grant),
        in_specs=specs,
        out_specs=jax.tree.map(lambda _: VM, outs),
        cost_estimate=pl.CostEstimate(flops=flops, bytes_accessed=1 << 20, transcendentals=0),
    )


def dot(a, b, dims=((1,), (0,))):
    return lax.dot_general(a, b, (dims, ((), ())), preferred_element_type=F32)


def column(start, width):
    return pl.ds(pl.multiple_of(start, LANES), width)


def pack_body(width, first, second, packed):
    away = (1 - lax.axis_index("tok")) * width
    packed[0] = first[:, column(away, width)]
    packed[1] = second[:, column(away, width)]


def pool_matrix(rows, across=False):
    parts = []
    for factor in POOLS:
        count = rows // factor
        dims = (rows, count) if across else (count, rows)
        token = lax.broadcasted_iota(jnp.int32, dims, 0 if across else 1)
        pooled = lax.broadcasted_iota(jnp.int32, dims, 1 if across else 0)
        low = pooled * factor
        inside = (token >= low) & (token < low + factor)
        parts.append(jnp.where(inside, 1.0 / factor, 0.0).astype(F32))
    return jnp.concatenate(parts, axis=1 if across else 0).astype(BF)


def own_start(width, whole_rows):
    return lax.axis_index("tok") * width if whole_rows else 0


def pool_body(rows, width, others, whole_rows, key_own, value_own, moved, *outs):
    start = own_start(width, whole_rows)
    matrix = pool_matrix(rows)
    for which, own in enumerate((key_own, value_own)):
        for block in range(others + 1):
            if block == 0:
                source = own[:, column(start, width)]
            else:
                source = moved[which, (block - 1) * rows : block * rows, :]
            pooled = dot(matrix, source).astype(BF)
            low = 0
            for factor, out in zip(POOLS, outs):
                count = rows // factor
                out[which, block * count : (block + 1) * count, :] = pooled[low : low + count]
                low += count


def attend_body(
    rows, width, others, whole_rows,
    video, age, query_own, key_own, value_own, grad_own, moved_kv, moved_qg, *rest
):
    pooled, outs = rest[:3], rest[3:]
    out_own, dquery_own, out_moved, dkv_own, dkv_moved = outs[:5]
    dpooled = outs[5:]
    start = own_start(width, whole_rows)
    here = lax.axis_index("frame")
    frame_rows = rows * (others + 1)
    biases = []
    for factor in POOLS:
        distance = jnp.int32(0)
        for a in range(3):
            distance = jnp.where(age[a] == factor, a + 1, distance)
        source = jnp.maximum(here - distance, 0)
        usable = (here >= distance) & (video[source] == video[here])
        biases.append(jnp.where(usable, 0.0, FAR).astype(F32))
    counts = [frame_rows // factor for factor in POOLS]
    used = frame_rows + sum(counts)
    padding = -used % LANES
    scale = HEAD**-0.5
    turn = scale * math.log2(math.e)
    block_chunks = 2 if (others + 1) % 2 == 0 else 1
    block_rows = block_chunks * rows

    def pair_step(pair, carry):
        offset = pair * LANES
        mine = column(start + offset, LANES)
        cols = column(offset, LANES)
        first_head = lax.broadcasted_iota(jnp.int32, (1, LANES), 1) < HEAD

        def key_rows_of(which, own):
            parts = [own[:, mine], moved_kv[which, :, cols]]
            parts += [p[which, :, cols] for p in pooled]
            if padding:
                parts.append(jnp.zeros((padding, LANES), BF))
            return jnp.concatenate(parts, axis=0)

        keys = key_rows_of(0, key_own)
        values = key_rows_of(1, value_own)
        keys_t = keys.T
        values_t = values.T
        dkeys = dvalues = None
        for block in range((others + 1) // block_chunks):
            chunks = range(block * block_chunks, (block + 1) * block_chunks)

            def query_rows_of(which, own):
                return jnp.concatenate(
                    [
                        own[:, mine] if c == 0 else moved_qg[which, (c - 1) * rows : c * rows, cols]
                        for c in chunks
                    ],
                    axis=0,
                )

            query = query_rows_of(0, query_own)
            grad = query_rows_of(1, grad_own)
            grad_t = grad.T
            results = []
            for head in range(2):
                keep = first_head if head == 0 else ~first_head
                query_h = jnp.where(keep, query, jnp.zeros_like(query))
                grad_h = jnp.where(keep, grad, jnp.zeros_like(grad))
                band = slice(head * HEAD, (head + 1) * HEAD)
                raw = dot(keys, query_h, ((1,), (1,)))
                parts = [raw[:frame_rows]]
                low = frame_rows
                for count, bias in zip(counts, biases):
                    parts.append(raw[low : low + count] + bias)
                    low += count
                if padding:
                    parts.append(jnp.full((padding, block_rows), FAR, F32))
                scores = jnp.concatenate(parts, axis=0)
                highest = jnp.max(scores, axis=0, keepdims=True)
                exponent = jnp.exp2((scores - highest) * turn)
                total = jnp.sum(exponent, axis=0, keepdims=True)
                weights = exponent * (1.0 / total)
                rounded = weights.astype(BF)
                out_t = dot(values_t[band], rounded).astype(BF)
                inner = jnp.sum(
                    grad_t[band].astype(F32) * out_t.astype(F32), axis=0, keepdims=True
                )
                dweights = dot(values, grad_h, ((1,), (1,)))
                dscores = (weights * (dweights - inner)).astype(BF)
                dquery_t = (dot(keys_t[band], dscores) * scale).astype(BF)
                results.append((query_h, grad_h, rounded, dscores, out_t, dquery_t))
            query_2, grad_2 = (
                jnp.concatenate([r[i] for r in results], axis=0) for i in (0, 1)
            )
            rounded_2, dscores_2 = (
                jnp.concatenate([r[i] for r in results], axis=1) for i in (2, 3)
            )
            out_2, dquery_2 = (
                jnp.concatenate([r[i] for r in results], axis=0).T for i in (4, 5)
            )
            dk = dot(dscores_2, query_2)
            dv = dot(rounded_2, grad_2)
            dkeys = dk if dkeys is None else dkeys + dk
            dvalues = dv if dvalues is None else dvalues + dv
            for place, c in enumerate(chunks):
                piece = slice(place * rows, (place + 1) * rows)
                if c == 0:
                    out_own[:, cols] = out_2[piece]
                    dquery_own[:, cols] = dquery_2[piece]
                else:
                    target = slice((c - 1) * rows, c * rows)
                    out_moved[0, target, cols] = out_2[piece]
                    out_moved[1, target, cols] = dquery_2[piece]
        for which, total in enumerate((dkeys * scale, dvalues)):
            dkv_own[which, :, cols] = total[:rows]
            dkv_moved[which, :, cols] = total[rows:frame_rows]
            low = frame_rows
            for count, target in zip(counts, dpooled):
                target[which, :, cols] = total[low : low + count].astype(BF)
                low += count
        return carry

    lax.fori_loop(0, width // LANES, pair_step, 0)


def spread_sum(rows, matrix, which, block, own_grads, back):
    pieces = []
    for factor, ref in zip(POOLS, back):
        count = rows // factor
        pieces.append(ref[which, block * count : (block + 1) * count, :])
    return (own_grads + dot(matrix, jnp.concatenate(pieces, axis=0))).astype(BF)


def combine_moved_body(rows, others, dkv_moved, *rest):
    back, moved = rest[:3], rest[3]
    matrix = pool_matrix(rows, across=True)
    for which in range(2):
        for block in range(1, others + 1):
            piece = slice((block - 1) * rows, block * rows)
            moved[which, piece, :] = spread_sum(
                rows, matrix, which, block, dkv_moved[which, piece, :], back
            )


def combine_own_body(rows, dkv_own, *rest):
    back, outs = rest[:3], rest[3:]
    matrix = pool_matrix(rows, across=True)
    for which, out in enumerate(outs):
        out[...] = spread_sum(rows, matrix, which, 0, dkv_own[which], back)


def finish_own_body(rows, width, dkv_own, *rest):
    back, (out_own, dquery_own, out_back), outs = rest[:3], rest[3:6], rest[6:]
    mine = column(lax.axis_index("tok") * width, width)
    away = column((1 - lax.axis_index("tok")) * width, width)
    for i, own in enumerate((out_own, dquery_own)):
        outs[i][:, mine] = own[...]
        outs[i][:, away] = out_back[i]
    matrix = pool_matrix(rows, across=True)
    for which in range(2):
        outs[2 + which][:, mine] = spread_sum(rows, matrix, which, 0, dkv_own[which], back)


def finish_moved_body(width, dkv_back, dkey_in, dvalue_in, dkey, dvalue, sems):
    away = column((1 - lax.axis_index("tok")) * width, width)
    copies = [
        pltpu.make_async_copy(dkv_back.at[i], out.at[:, away], sems.at[i])
        for i, out in enumerate((dkey, dvalue))
    ]
    for copy in copies:
        copy.start()
    for copy in copies:
        copy.wait()


def on_device(queries, key_rows, value_rows, grad_out, video_of_frame, age_pool):
    rows, columns = queries.shape[1:]
    ranks = lax.axis_size("tok")
    frames = lax.axis_size("frame")
    others = ranks - 1
    width = columns // ranks
    frame_rows = rows * ranks
    pair = ranks == 2
    swap = [(0, 1), (1, 0)]
    query, key, value, grad = (
        x.reshape(rows, columns) for x in (queries, key_rows, value_rows, grad_out)
    )
    if pair:
        pack = call(partial(pack_body, width), shape_of(2, rows, width), [VM, VM])
        moved_kv = lax.ppermute(pack(key, value), "tok", swap)
        moved_qg = lax.ppermute(pack(query, grad), "tok", swap)
    else:
        query, key, value, grad = (
            lax.all_to_all(x, "tok", split_axis=1, concat_axis=0, tiled=True)
            for x in (query, key, value, grad)
        )
        moved_kv = jnp.stack([key[rows:], value[rows:]])
        moved_qg = jnp.stack([query[rows:], grad[rows:]])
        query, key, value, grad = (x[:rows] for x in (query, key, value, grad))
    pooled_shapes = [shape_of(2, frame_rows // factor, width) for factor in POOLS]
    pooled = call(
        partial(pool_body, rows, width, others, pair), pooled_shapes, [VM] * 3
    )(key, value, moved_kv)

    where_two = jnp.where(age_pool[0] == 2, 0, jnp.where(age_pool[1] == 2, 1, 2))
    four_first = (age_pool[0] == 4) | ((age_pool[0] == 2) & (age_pool[1] == 4))
    order = (2 * where_two + jnp.where(four_first, 0, 1)).astype(jnp.int32)

    def shift(distances, sign, *blocks):
        return tuple(
            lax.ppermute(b, "frame", [(i, (i + sign * d) % frames) for i in range(frames)])
            for b, d in zip(blocks, distances)
        )

    pooled = lax.switch(order, [partial(shift, o, 1) for o in ORDERS], *pooled)
    heads = width // HEAD
    keys = frame_rows + sum(frame_rows // factor for factor in POOLS)
    results = call(
        partial(attend_body, rows, width, others, pair),
        [
            shape_of(rows, width),
            shape_of(rows, width),
            shape_of(2, others * rows, width),
            shape_of(2, rows, width, dtype=F32),
            shape_of(2, others * rows, width, dtype=F32),
            *pooled_shapes,
        ],
        [SM, SM] + [VM] * 9,
        flops=10 * frame_rows * keys * HEAD * heads,
        grant=32 << 20,
    )(video_of_frame, age_pool, query, key, value, grad, moved_kv, moved_qg, *pooled)
    out_own, dquery_own, out_moved, dkv_own, dkv_moved = results[:5]
    if pair:
        out_back = lax.ppermute(out_moved, "tok", swap)
    back = lax.switch(order, [partial(shift, o, -1) for o in ORDERS], *results[5:])
    moved_shape = shape_of(2, others * rows, width)
    dkv_moved = call(partial(combine_moved_body, rows, others), moved_shape, [VM] * 4)(
        dkv_moved, *back
    )
    if pair:
        dkv_back = lax.ppermute(dkv_moved, "tok", swap)
        whole = shape_of(rows, columns)
        outs = call(partial(finish_own_body, rows, width), [whole] * 4, [VM] * 7)(
            dkv_own, *back, out_own, dquery_own, out_back
        )
        dkey, dvalue = pl.pallas_call(
            partial(finish_moved_body, width),
            out_shape=[whole] * 2,
            in_specs=[VM, ANY, ANY],
            out_specs=[ANY, ANY],
            scratch_shapes=[pltpu.SemaphoreType.DMA((2,))],
            input_output_aliases={1: 0, 2: 1},
            compiler_params=pltpu.CompilerParams(vmem_limit_bytes=16 << 20),
        )(dkv_back, outs[2], outs[3])
        outs = (outs[0], outs[1], dkey, dvalue)
    else:
        dkey_own, dvalue_own = call(
            partial(combine_own_body, rows), [shape_of(rows, width)] * 2, [VM] * 4
        )(dkv_own, *back)
        outs = [
            lax.all_to_all(
                jnp.concatenate([own, moved], axis=0), "tok", split_axis=0, concat_axis=1, tiled=True
            )
            for own, moved in (
                (out_own, out_moved[0]),
                (dquery_own, out_moved[1]),
                (dkey_own, dkv_moved[0]),
                (dvalue_own, dkv_moved[1]),
            )
        ]
    return tuple(x.reshape(1, rows, columns) for x in outs)


def solution(mesh):
    rows = P("frame", "tok", None)
    return jax.shard_map(
        on_device,
        mesh=mesh,
        in_specs=(rows,) * 4 + (P(), P()),
        out_specs=(rows,) * 4,
        check_vma=False,
    )
```
